256 devices in a mesh: seq: 32 (over y, z_hi, core), head: 8 (over x, z_lo).
Axes of the slice: x: 4, y: 4, z: 8 (z_hi: 4, z_lo: 2; z = z_hi * 2 + z_lo), core: 2. Of those that a mesh axis runs over, the one named last changes fastest.
Arguments:
- queries: bfloat16 [16384, 4096], P('seq', 'head'), may hold values from -20 to 20
- key_rows: bfloat16 [16384, 2048], P('seq', 'head'), may hold values from -20 to 20
- values: bfloat16 [16384, 2048], P('seq', 'head'), may hold values from -24 to 24
- out_weight: bfloat16 [4096, 5376], P('head'), may hold values from -0.09375 to 0.09375
Outputs:
- projected: bfloat16 [16384, 5376], P(('seq', 'head'))
The draws below stay inside these ranges and needn't reach their ends.
All inputs are finite; a program needn't handle non-finite values.
Results may differ from the reference program's by a relative error of at most 0.019.
Values may be sent and summed in bfloat16 or wider, within the bound.
No kernel may reach another device: no remote copies, remote signals or barrier semaphores. Data moves between devices by JAX's collectives and lax.ppermute only.
A program may use at most 128 MiB of HBM per device.

```python
import math
import jax
import jax.numpy as jnp
from jax import lax

D = 5376
QH = 32
KVH = 16
HD = 128
TOKENS = 16384


def query_key_pair(key):
    base_key = jax.random.fold_in(key, 101)
    query_key, rows_key = jax.random.split(base_key, 2)
    queries = 1.6 * jnp.clip(jax.random.normal(query_key, (TOKENS, QH * HD), jnp.float32), -4.0, 4.0)
    key_rows = 1.6 * jnp.clip(jax.random.normal(rows_key, (TOKENS, KVH * HD), jnp.float32), -4.0, 4.0)
    return (queries, key_rows)


def draw_queries(key, part):
    return query_key_pair(key)[0].astype(jnp.bfloat16)


def draw_key_rows(key, part):
    return query_key_pair(key)[1].astype(jnp.bfloat16)


def block_levels(own_key, shape, cuts, smallest, largest):
    def one(dim, parts):
        draws = jax.random.uniform(jax.random.fold_in(jax.random.fold_in(own_key, 6), dim), (parts,), jnp.float32, smallest / len(cuts), largest / len(cuts))
        return jnp.repeat(jnp.exp(draws), shape[dim] // parts).reshape((-1,) + (1,) * (len(shape) - dim - 1))

    level = one(*cuts[0])
    for cut in cuts[1:]:
        level = level * one(*cut)
    return level


def noise(own_key, dims, spread, reach, cuts=(), kind=jnp.bfloat16):
    array = jax.random.normal(own_key, dims, jnp.float32) * spread
    if len(cuts) > 0:
        array = block_levels(own_key, dims, cuts, -0.22, 0.18) * array
    return jnp.clip(array, min=-reach, max=reach).astype(kind)


def setup_inputs(seed: int = 0) -> dict:
    arg_keys = jax.random.split(jax.random.key(seed), 5)
    return {
        "queries": draw_queries(jax.random.fold_in(arg_keys[4], 71), 0),
        "key_rows": draw_key_rows(jax.random.fold_in(arg_keys[4], 71), 0),
        "values": noise(arg_keys[2], (TOKENS, KVH * HD), 4.0, 24.0, ((0, 32), (1, 8))),
        "out_weight": noise(arg_keys[3], (QH * HD, D), (QH * HD) ** -0.5, 0.09375, ((0, 8),)),
    }


attn_scale = 168.0 ** -0.5
neg_fill = -1e30


def reference(queries, key_rows, values, out_weight):
    per_group = QH // KVH
    query_grid = queries.reshape(TOKENS, KVH, per_group, HD)
    key_grid = key_rows.reshape(TOKENS, KVH, HD)
    value_grid = values.reshape(TOKENS, KVH, HD)
    block_rows = math.gcd(TOKENS, 512)
    blocks = TOKENS // block_rows
    order_index = jnp.arange(blocks * KVH, dtype=jnp.int32)

    def one_block(index):
        block_id = (index // KVH).astype(jnp.int32)
        head_id = (index % KVH).astype(jnp.int32)
        zero = jnp.int32(0)
        query_part = lax.dynamic_slice(query_grid, (block_id * block_rows, head_id, zero, zero), (block_rows, 1, per_group, HD))[:, 0]
        key_part = lax.dynamic_slice(key_grid, (zero, head_id, zero), (TOKENS, 1, HD))[:, 0]
        value_part = lax.dynamic_slice(value_grid, (zero, head_id, zero), (TOKENS, 1, HD))[:, 0]
        scores = jnp.einsum("qgd,kd->gqk", query_part.astype(jnp.float32), key_part.astype(jnp.float32)) * attn_scale
        query_pos = block_id * block_rows + jnp.arange(block_rows, dtype=jnp.int32)
        key_pos = jnp.arange(TOKENS, dtype=jnp.int32)
        allowed = key_pos[None, :] <= query_pos[:, None]
        scores = jnp.where(allowed[None], scores, neg_fill)
        row_max = jnp.max(scores, axis=-1, keepdims=True)
        weights = jnp.where(allowed[None], jnp.exp(scores - row_max), 0.0)
        row_sum = jnp.sum(weights, axis=-1)
        rounded = weights.astype(jnp.bfloat16)
        mixed = jnp.einsum("gqk,kd->gqd", rounded.astype(jnp.float32), value_part.astype(jnp.float32))
        return (mixed / row_sum[..., None]).astype(jnp.bfloat16)

    outputs = lax.map(one_block, order_index)
    outputs = outputs.reshape(blocks, KVH, per_group, block_rows, HD)
    attended = outputs.transpose(0, 3, 1, 2, 4).reshape(TOKENS, QH * HD)
    return jnp.dot(attended, out_weight, preferred_element_type=jnp.float32).astype(jnp.bfloat16)
```

```python
import jax
import jax.numpy as jnp
from jax import lax
from jax.experimental import pallas as pl
from jax.experimental.pallas import tpu as pltpu
from jax.sharding import Mesh
from jax.sharding import PartitionSpec as P

HD = 128
PAIR = 2 * HD
LOG2E = 1.4426950408889634
query_scale = 168.0 ** (-0.5) * LOG2E
neg_fill = -1e30
CHUNK = 512
TILE = 256


def moved(value, axes, mapping):
    names = axes if isinstance(axes, tuple) else (axes,)
    sizes = [lax.axis_size(name) for name in names]
    pairs = []
    total = 1
    for size in sizes:
        total *= size
    for source in range(total):
        coords, rest = [], source
        for size in reversed(sizes):
            coords.append(rest % size)
            rest //= size
        target = 0
        for size, at in zip(sizes, mapping(tuple(reversed(coords)))):
            target = target * size + at % size
        pairs.append((source, target))
    return lax.ppermute(value, axes, pairs)


def attend_kernel(lo, hi, diag, q_ref, kv_ref, out_ref, lse_ref, m_ref, l_ref, acc_ref):
    tasks, _, rows = q_ref.shape
    half = rows // 2
    span = kv_ref.shape[1] // 2
    per_span = span // CHUNK

    def step(task, chunk, masked):
        which = chunk // per_span
        at = pl.multiple_of((chunk % per_span) * CHUNK, CHUNK)
        keys = kv_ref[which, pl.ds(at, CHUNK), :]
        keys_twice = jnp.concatenate([keys, keys], axis=1)
        values_t = jnp.concatenate(
            [
                kv_ref[which, pl.ds(pl.multiple_of(span + at, CHUNK) + i * HD, HD), :]
                for i in range(CHUNK // HD)
            ],
            axis=1,
        )
        for r in range(rows // TILE):
            cols = pl.ds(r * TILE, TILE)
            scores = jnp.dot(keys_twice, q_ref[task, :, cols], preferred_element_type=jnp.float32)
            if masked:
                key_pos = lax.broadcasted_iota(jnp.int32, (CHUNK, TILE), 0)
                row_pos = lax.broadcasted_iota(jnp.int32, (CHUNK, TILE), 1) + (r * TILE) % half
                scores = jnp.where(key_pos <= row_pos, scores, neg_fill)
            old_max = m_ref[:, cols]
            new_max = jnp.maximum(old_max, jnp.max(scores, axis=0, keepdims=True))
            weights = jnp.exp2(scores - new_max)
            factor = jnp.exp2(old_max - new_max)
            l_ref[:, cols] = l_ref[:, cols] * factor + jnp.sum(weights, axis=0, keepdims=True)
            m_ref[:, cols] = new_max
            acc_ref[:, cols] = acc_ref[:, cols] * factor + jnp.dot(
                values_t, weights.astype(jnp.bfloat16), preferred_element_type=jnp.float32
            )

    def one_task(t, _):
        m_ref[...] = jnp.full_like(m_ref, neg_fill)
        l_ref[...] = jnp.zeros_like(l_ref)
        acc_ref[...] = jnp.zeros_like(acc_ref)

        def body(chunk, _):
            step(t, chunk, False)
            return 0

        lax.fori_loop(lo[t], hi[t], body, 0)

        @pl.when(diag[t] > 0)
        def _():
            step(t, hi[t], True)

        total = l_ref[...]
        some = total > 0.0
        safe = jnp.where(some, total, 1.0)
        lse_ref[t] = jnp.where(some, m_ref[...] + jnp.log2(safe), neg_fill)
        out = acc_ref[...] / safe
        for h in range(2):
            out_ref[t, :, h * HD : (h + 1) * HD] = out[:, h * half : (h + 1) * half].T.astype(
                out_ref.dtype
            )
        return 0

    lax.fori_loop(0, tasks, one_task, 0)


def attend(lo, hi, diag, q, kv, share):
    tasks, _, rows = q.shape
    smem = pl.BlockSpec(memory_space=pltpu.SMEM)
    vmem = pl.BlockSpec(memory_space=pltpu.VMEM)
    return pl.pallas_call(
        attend_kernel,
        out_shape=(
            jax.ShapeDtypeStruct((tasks, rows // 2, PAIR), jnp.bfloat16),
            jax.ShapeDtypeStruct((tasks, 1, rows), jnp.float32),
        ),
        in_specs=[smem, smem, smem, vmem, vmem],
        out_specs=(vmem, vmem),
        scratch_shapes=[
            pltpu.VMEM((1, rows), jnp.float32),
            pltpu.VMEM((1, rows), jnp.float32),
            pltpu.VMEM((HD, rows), jnp.float32),
        ],
        compiler_params=pltpu.CompilerParams(vmem_limit_bytes=40 * 2**20),
        cost_estimate=pl.CostEstimate(
            flops=share * 16384 * 1024 * HD * 4, bytes_accessed=9_000_000, transcendentals=0
        ),
    )(lo, hi, diag, q, kv)


def packed_queries(q):
    tokens = q.shape[0]
    scaled = q.astype(jnp.float32) * query_scale
    scaled = scaled.reshape(tokens, 2, HD).transpose(2, 1, 0).reshape(HD, 2 * tokens)
    high = lax.reduce_precision(scaled, 8, 7)
    low = scaled - high
    return jnp.concatenate([high, low], axis=0).astype(jnp.bfloat16)


def values_in_blocks(v):
    tokens = v.shape[0]
    return v.reshape(tokens // HD, HD, HD).transpose(0, 2, 1).reshape(tokens, HD)


def per_device(queries, key_rows, values, out_weight):
    core = lax.axis_index("c")
    x = lax.axis_index("x")
    zl = lax.axis_index("zl")
    spans_y, spans_z = lax.axis_size("y"), lax.axis_size("zh")
    spans = spans_y * spans_z
    span = lax.axis_index("y") * spans_z + lax.axis_index("zh")
    rows = queries.shape[0]
    width = out_weight.shape[1]
    half_width = width // 2

    mine = jnp.concatenate(
        [
            lax.dynamic_slice_in_dim(queries, core * PAIR, PAIR, 1),
            lax.dynamic_slice_in_dim(key_rows, core * HD, HD, 1),
            lax.dynamic_slice_in_dim(values, core * HD, HD, 1),
        ],
        axis=1,
    )
    theirs = jnp.concatenate(
        [
            lax.dynamic_slice_in_dim(queries, (1 - core) * PAIR, PAIR, 1),
            lax.dynamic_slice_in_dim(key_rows, (1 - core) * HD, HD, 1),
            lax.dynamic_slice_in_dim(values, (1 - core) * HD, HD, 1),
        ],
        axis=1,
    )
    got = moved(theirs, "c", lambda at: (1 - at[0],))
    first = jnp.where(core == 0, mine, got)
    second = jnp.where(core == 0, got, mine)

    kv_own = jnp.concatenate(
        [
            first[:, PAIR : PAIR + HD],
            second[:, PAIR : PAIR + HD],
            values_in_blocks(first[:, PAIR + HD :]),
            values_in_blocks(second[:, PAIR + HD :]),
        ],
        axis=0,
    )
    kv = lax.all_gather(kv_own, ("y", "zh"), axis=0)

    mirror = lambda at: (spans_y - 1 - at[0], spans_z - 1 - at[1])
    lent = moved(second[:, :PAIR], ("y", "zh"), mirror)

    own_w = lax.dynamic_slice_in_dim(out_weight, core * half_width, half_width, 1)
    part = own_w.shape[0] // 2
    w_left = moved(own_w, "x", lambda at: (at[0] + 1,))
    w_right = moved(own_w, "x", lambda at: (at[0] - 1,))
    w_far_top = moved(w_left[:part], "x", lambda at: (at[0] + 1,))
    w_far_low = moved(w_right[part:], "x", lambda at: (at[0] - 1,))

    lent_len = jnp.maximum(2 * span - (spans - 1), 0)
    taken_len = jnp.maximum(spans - 1 - 2 * span, 0)
    ints = lambda *v: jnp.stack([jnp.asarray(e, jnp.int32) for e in v])
    lent_out, lent_lse = attend(
        ints(0), ints(2 * taken_len), ints(0), packed_queries(lent)[None], kv, 1
    )
    back_out = moved(lent_out[0], ("y", "zh"), mirror)
    back_lse = moved(lent_lse[0], ("y", "zh"), mirror)
    q_own = jnp.stack([packed_queries(first[:, :PAIR]), packed_queries(second[:, :PAIR])])
    own_out, own_lse = attend(
        ints(0, 2 * lent_len), ints(2 * span, 2 * span + 1), ints(1, 1), q_own, kv, 1
    )
    back_lse = jnp.where(lent_len > 0, back_lse[0], neg_fill)
    joint = jnp.maximum(own_lse[1, 0], back_lse)
    own_part = jnp.exp2(own_lse[1, 0] - joint)
    back_part = jnp.exp2(back_lse - joint)
    total = own_part + back_part

    def by_row(a):
        return jnp.repeat(a.reshape(2, rows).T, HD, axis=1)

    merged = own_out[1].astype(jnp.float32) * by_row(own_part / total) + back_out.astype(
        jnp.float32
    ) * by_row(back_part / total)
    attended = jnp.stack([own_out[0], merged.astype(jnp.bfloat16)])

    groups = lax.axis_size("x")
    piece = rows // groups
    by_x = attended.reshape(2, groups, piece, PAIR).transpose(1, 0, 2, 3)
    by_x = by_x.reshape(groups, 2 * piece, PAIR)

    def towards(k):
        block = lax.dynamic_index_in_dim(by_x, (x + k) % groups, 0, keepdims=False)
        return block if k == 0 else moved(block, "x", lambda at: (at[0] + k,))

    heads_mine = jnp.concatenate([towards(k) for k in range(groups)], axis=1)
    heads_other = moved(heads_mine, "c", lambda at: (1 - at[0],))
    of_core = [jnp.where(core == 0, heads_mine, heads_other), jnp.where(core == 0, heads_other, heads_mine)]
    w_terms = [own_w, w_left, jnp.concatenate([w_far_top, w_far_low], axis=0), w_right]
    partial = 0.0
    for k in range(groups):
        lhs = jnp.concatenate([half[:, k * PAIR : (k + 1) * PAIR] for half in of_core], axis=1)
        partial = partial + jnp.dot(lhs, w_terms[k], preferred_element_type=jnp.float32)

    partial = partial.reshape(2, 2, piece // 2, half_width)

    def block_of(c_at, z_at):
        return lax.dynamic_slice(partial, (c_at, z_at, 0, 0), (1, 1, piece // 2, half_width))[0, 0]

    send_z = block_of(core, 1 - zl).astype(jnp.bfloat16)
    send_c = block_of(1 - core, zl).astype(jnp.bfloat16)
    send_cz = block_of(1 - core, 1 - zl).astype(jnp.bfloat16)
    got_z = moved(send_z, "zl", lambda at: (1 - at[0],))
    got_cz = moved(send_cz, ("c", "zl"), lambda at: (1 - at[0], 1 - at[1]))
    got_c = moved(send_c, "c", lambda at: (1 - at[0],))
    mine_cols = (block_of(core, zl) + got_z.astype(jnp.float32)).astype(jnp.bfloat16)
    other_cols = (got_c.astype(jnp.float32) + got_cz.astype(jnp.float32)).astype(jnp.bfloat16)
    return jnp.where(
        core == 0,
        jnp.concatenate([mine_cols, other_cols], axis=1),
        jnp.concatenate([other_cols, mine_cols], axis=1),
    )


def solution(mesh):
    names = ("y", "zh", "c", "x", "zl")
    torus = Mesh(mesh.devices.reshape(4, 4, 2, 4, 2), names)
    seq, head = ("y", "zh", "c"), ("x", "zl")
    in_specs = (P(seq, head), P(seq, head), P(seq, head), P(head, None))
    out_specs = P(seq + head, None)
    return jax.shard_map(
        per_device, mesh=torus, in_specs=in_specs, out_specs=out_specs, check_vma=False
    )
```

```python
import jax
import jax.numpy as jnp
from jax import lax
from jax.experimental import pallas as pl
from jax.experimental.pallas import tpu as pltpu
from jax.sharding import Mesh
from jax.sharding import PartitionSpec as P

HD = 128
PAIR = 2 * HD
LOG2E = 1.4426950408889634
query_scale = 168.0 ** (-0.5) * LOG2E
neg_fill = -1e30
TILE = 256
PLACES = (
    [(4 * dy, 0) for dy in (0, 1, 3)]
    + [(8, 0), (8, 1)]
    + [(4 * dy + dz, 0) for dz in (1, 3) for dy in (0, 1, 3, 2)]
    + [(4 * dy + 2, 0) for dy in (0, 1, 3)]
    + [(10, 0), (10, 1)]
)


def moved(value, axes, mapping):
    names = axes if isinstance(axes, tuple) else (axes,)
    sizes = [lax.axis_size(name) for name in names]
    pairs = []
    total = 1
    for size in sizes:
        total *= size
    for source in range(total):
        coords, rest = [], source
        for size in reversed(sizes):
            coords.append(rest % size)
            rest //= size
        target = 0
        for size, at in zip(sizes, mapping(tuple(reversed(coords)))):
            target = target * size + at % size
        pairs.append((source, target))
    return lax.ppermute(value, axes, pairs)


def attend_kernel(lo, hi, diag, slots, q_ref, *refs):
    pieces, (out_ref, lse_ref, kv_ref, m_ref, l_ref, acc_ref, sems) = refs[:-7], refs[-7:]
    tasks, _, rows = q_ref.shape
    half = rows // 2
    span = kv_ref.shape[1] // 2

    copies = [
        pltpu.make_async_copy(
            piece, kv_ref.at[slot, pl.ds(part * span, piece.shape[0]), :], sems.at[i]
        )
        for i, (piece, (slot, part)) in enumerate(zip(pieces, PLACES))
    ]
    for copy in copies:
        copy.start()
    for copy in copies:
        copy.wait()

    def step(task, at_span, masked):
        slot = slots[at_span]
        keys = kv_ref[slot, pl.ds(0, span), :]
        keys_twice = jnp.concatenate([keys, keys], axis=1)
        values_t = jnp.concatenate(
            [kv_ref[slot, pl.ds(span + i * HD, HD), :] for i in range(span // HD)], axis=1
        )
        tiles = [pl.ds(r * TILE, TILE) for r in range(rows // TILE)]
        all_scores = [
            jnp.dot(keys_twice, q_ref[task, :, cols], preferred_element_type=jnp.float32)
            for cols in tiles
        ]
        for r, (cols, scores) in enumerate(zip(tiles, all_scores)):
            if masked:
                key_pos = lax.broadcasted_iota(jnp.int32, (span, TILE), 0)
                row_pos = lax.broadcasted_iota(jnp.int32, (span, TILE), 1) + (r * TILE) % half
                scores = jnp.where(key_pos <= row_pos + task * half, scores, neg_fill)
            old_max = m_ref[:, cols]
            new_max = jnp.maximum(old_max, jnp.max(scores, axis=0, keepdims=True))
            weights = jnp.exp2(scores - new_max)
            factor = jnp.exp2(old_max - new_max)
            l_ref[:, cols] = l_ref[:, cols] * factor + jnp.sum(weights, axis=0, keepdims=True)
            m_ref[:, cols] = new_max
            acc_ref[:, cols] = acc_ref[:, cols] * factor + jnp.dot(
                values_t, weights.astype(jnp.bfloat16), preferred_element_type=jnp.float32
            )

    def one_task(t, _):
        m_ref[...] = jnp.full_like(m_ref, neg_fill)
        l_ref[...] = jnp.zeros_like(l_ref)
        acc_ref[...] = jnp.zeros_like(acc_ref)

        def body(at_span, _):
            step(t, at_span, False)
            return 0

        lax.fori_loop(lo[t], hi[t], body, 0)

        @pl.when(diag[t] > 0)
        def _():
            step(t, hi[t], True)

        total = l_ref[...]
        some = total > 0.0
        safe = jnp.where(some, total, 1.0)
        lse_ref[t] = jnp.where(some, m_ref[...] + jnp.log2(safe), neg_fill)
        out = acc_ref[...] / safe
        for h in range(2):
            out_ref[t, :, h * HD : (h + 1) * HD] = out[:, h * half : (h + 1) * half].T.astype(
                out_ref.dtype
            )
        return 0

    lax.fori_loop(0, tasks, one_task, 0)


def attend(lo, hi, diag, slots, q, pieces):
    tasks, _, rows = q.shape
    smem = pl.BlockSpec(memory_space=pltpu.SMEM)
    vmem = pl.BlockSpec(memory_space=pltpu.VMEM)
    hbm = pl.BlockSpec(memory_space=pltpu.MemorySpace.HBM)
    return pl.pallas_call(
        attend_kernel,
        out_shape=(
            jax.ShapeDtypeStruct((tasks, rows // 2, PAIR), jnp.bfloat16),
            jax.ShapeDtypeStruct((tasks, 1, rows), jnp.float32),
        ),
        in_specs=[smem] * 4 + [vmem] + [hbm] * len(pieces),
        out_specs=(vmem, vmem),
        scratch_shapes=[
            pltpu.VMEM((16,) + pieces[0].shape, jnp.bfloat16),
            pltpu.VMEM((1, rows), jnp.float32),
            pltpu.VMEM((1, rows), jnp.float32),
            pltpu.VMEM((HD, rows), jnp.float32),
            pltpu.SemaphoreType.DMA((len(pieces),)),
        ],
        compiler_params=pltpu.CompilerParams(vmem_limit_bytes=48 * 2**20),
        cost_estimate=pl.CostEstimate(
            flops=16384 * 1024 * HD * 4, bytes_accessed=9_000_000, transcendentals=0
        ),
    )(lo, hi, diag, slots, q, *pieces)


def packed_queries(q):
    tokens = q.shape[0]
    scaled = q.astype(jnp.float32) * query_scale
    scaled = scaled.reshape(tokens, 2, HD).transpose(2, 1, 0).reshape(HD, 2 * tokens)
    high = lax.reduce_precision(scaled, 8, 7)
    low = scaled - high
    return jnp.concatenate([high, low], axis=0).astype(jnp.bfloat16)


def values_in_blocks(v):
    tokens = v.shape[0]
    return v.reshape(tokens // HD, HD, HD).transpose(0, 2, 1).reshape(tokens, HD)


def layer(queries, key_rows, values, out_weight):
    core = lax.axis_index("c")
    x = lax.axis_index("x")
    zl = lax.axis_index("zl")
    spans_y, spans_z = lax.axis_size("y"), lax.axis_size("zh")
    spans = spans_y * spans_z
    span = lax.axis_index("y") * spans_z + lax.axis_index("zh")
    rows = queries.shape[0]
    width = out_weight.shape[1]
    half_width = width // 2

    mine = jnp.concatenate(
        [
            lax.dynamic_slice_in_dim(queries, core * PAIR, PAIR, 1),
            lax.dynamic_slice_in_dim(key_rows, core * HD, HD, 1),
            lax.dynamic_slice_in_dim(values, core * HD, HD, 1),
        ],
        axis=1,
    )
    theirs = jnp.concatenate(
        [
            lax.dynamic_slice_in_dim(queries, (1 - core) * PAIR, PAIR, 1),
            lax.dynamic_slice_in_dim(key_rows, (1 - core) * HD, HD, 1),
            lax.dynamic_slice_in_dim(values, (1 - core) * HD, HD, 1),
        ],
        axis=1,
    )
    got = moved(theirs, "c", lambda at: (1 - at[0],))
    first = jnp.where(core == 0, mine, got)
    second = jnp.where(core == 0, got, mine)

    kv_own = jnp.concatenate(
        [
            first[:, PAIR : PAIR + HD],
            second[:, PAIR : PAIR + HD],
            values_in_blocks(first[:, PAIR + HD :]),
            values_in_blocks(second[:, PAIR + HD :]),
        ],
        axis=0,
    )
    y_up = lambda a: moved(a, "y", lambda at: (at[0] + 1,))
    y_down = lambda a: moved(a, "y", lambda at: (at[0] - 1,))
    z_up = lambda a: moved(a, "zh", lambda at: (at[0] + 1,))
    z_down = lambda a: moved(a, "zh", lambda at: (at[0] - 1,))
    own_kv = kv_own
    z1, z3 = z_up(own_kv), z_down(own_kv)
    y1, y3 = y_up(own_kv), y_down(own_kv)
    mirror = lambda at: (spans_y - 1 - at[0], spans_z - 1 - at[1])
    lent = moved(second[:, :PAIR], ("y", "zh"), mirror)
    own_w = lax.dynamic_slice_in_dim(out_weight, core * half_width, half_width, 1)
    part = own_w.shape[0] // 2
    w_left = moved(own_w, "x", lambda at: (at[0] + 1,))
    w_right = moved(own_w, "x", lambda at: (at[0] - 1,))

    size = own_kv.shape[0] // 2
    pieces = [own_kv, y1, y3, y_up(y1[:size]), y_down(y3[size:])]
    z2 = jnp.concatenate([z_up(z1[:size]), z_down(z3[size:])], axis=0)
    z1_up, z1_down = y_up(z1), y_down(z1)
    z3_up, z3_down = y_up(z3), y_down(z3)
    pieces += [z1, z1_up, z1_down, y_up(z1_up)]
    pieces += [z3, z3_up, z3_down, y_down(z3_down)]
    z2_up, z2_down = y_up(z2), y_down(z2)
    pieces += [z2, z2_up, z2_down, y_up(z2_up[:size]), y_down(z2_down[size:])]
    w_left, w_right, *_ = lax.optimization_barrier((w_left, w_right, z1_up, z1_down, z3_up, z3_down))
    w_far_top = moved(w_left[:part], "x", lambda at: (at[0] + 1,))
    w_far_low = moved(w_right[part:], "x", lambda at: (at[0] - 1,))

    lent_len = jnp.maximum(2 * span - (spans - 1), 0)
    taken_len = jnp.maximum(spans - 1 - 2 * span, 0)
    ints = lambda *v: jnp.stack([jnp.asarray(e, jnp.int32) for e in v])
    order = jnp.arange(spans, dtype=jnp.int32)
    slots = (lax.axis_index("y") - order // spans_z) % spans_y * 4
    slots = (slots + (lax.axis_index("zh") - order % spans_z) % spans_z).astype(jnp.int32)
    q_all = jnp.stack([packed_queries(a) for a in (first[:, :PAIR], second[:, :PAIR], lent)])
    out, lse = attend(
        ints(0, lent_len, 0), ints(span, span, taken_len), ints(1, 1, 0), slots, q_all, pieces
    )
    back_out = moved(out[2], ("y", "zh"), mirror)
    back_lse = moved(lse[2], ("y", "zh"), mirror)
    back_lse = jnp.where(lent_len > 0, back_lse[0], neg_fill)
    joint = jnp.maximum(lse[1, 0], back_lse)
    own_part = jnp.exp2(lse[1, 0] - joint)
    back_part = jnp.exp2(back_lse - joint)
    total = own_part + back_part

    def by_row(a):
        return jnp.repeat(a.reshape(2, rows).T, HD, axis=1)

    merged = out[1].astype(jnp.float32) * by_row(own_part / total) + back_out.astype(
        jnp.float32
    ) * by_row(back_part / total)
    attended = jnp.stack([out[0], merged.astype(jnp.bfloat16)])

    groups = lax.axis_size("x")
    piece = rows // groups
    by_x = attended.reshape(2, groups, piece, PAIR).transpose(1, 0, 2, 3)
    by_x = by_x.reshape(groups, 2 * piece, PAIR)

    def towards(k):
        block = lax.dynamic_index_in_dim(by_x, (x + k) % groups, 0, keepdims=False)
        return block if k == 0 else moved(block, "x", lambda at: (at[0] + k,))

    heads_mine = jnp.concatenate([towards(k) for k in range(groups)], axis=1)
    heads_other = moved(heads_mine, "c", lambda at: (1 - at[0],))
    of_core = [jnp.where(core == 0, heads_mine, heads_other), jnp.where(core == 0, heads_other, heads_mine)]
    w_terms = [own_w, w_left, jnp.concatenate([w_far_top, w_far_low], axis=0), w_right]
    partial = 0.0
    for k in range(groups):
        lhs = jnp.concatenate([half[:, k * PAIR : (k + 1) * PAIR] for half in of_core], axis=1)
        partial = partial + jnp.dot(lhs, w_terms[k], preferred_element_type=jnp.float32)

    partial = partial.reshape(2, 2, piece // 2, half_width)

    def block_of(c_at, z_at):
        return lax.dynamic_slice(partial, (c_at, z_at, 0, 0), (1, 1, piece // 2, half_width))[0, 0]

    send_z = block_of(core, 1 - zl).astype(jnp.bfloat16)
    send_c = block_of(1 - core, zl).astype(jnp.bfloat16)
    send_cz = block_of(1 - core, 1 - zl).astype(jnp.bfloat16)
    got_z = moved(send_z, "zl", lambda at: (1 - at[0],))
    got_cz = moved(send_cz, ("c", "zl"), lambda at: (1 - at[0], 1 - at[1]))
    got_c = moved(send_c, "c", lambda at: (1 - at[0],))
    mine_cols = (block_of(core, zl) + got_z.astype(jnp.float32)).astype(jnp.bfloat16)
    other_cols = (got_c.astype(jnp.float32) + got_cz.astype(jnp.float32)).astype(jnp.bfloat16)
    return jnp.where(
        core == 0,
        jnp.concatenate([mine_cols, other_cols], axis=1),
        jnp.concatenate([other_cols, mine_cols], axis=1),
    )


def solution(mesh):
    names = ("y", "zh", "c", "x", "zl")
    torus = Mesh(mesh.devices.reshape(4, 4, 2, 4, 2), names)
    seq, head = ("y", "zh", "c"), ("x", "zl")
    in_specs = (P(seq, head), P(seq, head), P(seq, head), P(head, None))
    out_specs = P(seq + head, None)
    return jax.shard_map(layer, mesh=torus, in_specs=in_specs, out_specs=out_specs, check_vma=False)
```

```python
import jax
import jax.numpy as jnp
from jax import lax
from jax.experimental import pallas as pl
from jax.experimental.pallas import tpu as pltpu
from jax.sharding import Mesh
from jax.sharding import PartitionSpec as P

HD = 128
PAIR = 2 * HD
LOG2E = 1.4426950408889634
query_scale = 168.0 ** (-0.5) * LOG2E
neg_fill = -1e30
TILE = 256
PLACES = (
    [(4 * dy, 0) for dy in (0, 1, 3, 2)]
    + [(4 * dy + dz, 0) for dz in (1, 3) for dy in (0, 1, 3, 2)]
    + [(4 * dy + 2, 0) for dy in (0, 1, 3)]
    + [(10, 0), (10, 1)]
)


def moved(value, axes, mapping):
    names = axes if isinstance(axes, tuple) else (axes,)
    sizes = [lax.axis_size(name) for name in names]
    pairs = []
    total = 1
    for size in sizes:
        total *= size
    for source in range(total):
        coords, rest = [], source
        for size in reversed(sizes):
            coords.append(rest % size)
            rest //= size
        target = 0
        for size, at in zip(sizes, mapping(tuple(reversed(coords)))):
            target = target * size + at % size
        pairs.append((source, target))
    return lax.ppermute(value, axes, pairs)


def attend_kernel(lo, hi, diag, slots, q_ref, *refs):
    pieces, (out_ref, lse_ref, kv_ref, s_ref, m_ref, l_ref, acc_ref, sems) = refs[:-8], refs[-8:]
    tasks, _, rows = q_ref.shape
    half = rows // 2
    span = kv_ref.shape[1] // 2

    copies = [
        pltpu.make_async_copy(
            piece, kv_ref.at[slot, pl.ds(part * span, piece.shape[0]), :], sems.at[i]
        )
        for i, (piece, (slot, part)) in enumerate(zip(pieces, PLACES))
    ]
    for copy in copies:
        copy.start()
    for copy in copies:
        copy.wait()

    tiles = [pl.ds(r * TILE, TILE) for r in range(rows // TILE)]

    def keys_twice(at_span):
        keys = kv_ref[slots[at_span], pl.ds(0, span), :]
        return jnp.concatenate([keys, keys], axis=1)

    def scores_of(keys, task, cols):
        return jnp.dot(keys, q_ref[task, :, cols], preferred_element_type=jnp.float32)

    def step(task, at_span, last):
        slot = slots[at_span]
        values_t = jnp.concatenate(
            [kv_ref[slot, pl.ds(span + i * HD, HD), :] for i in range(span // HD)], axis=1
        )
        keys = None if last else keys_twice(at_span + 1)
        for r, cols in enumerate(tiles):
            scores = s_ref[:, cols]
            following = None if last else scores_of(keys, task, cols)
            if last:
                key_pos = lax.broadcasted_iota(jnp.int32, (span, TILE), 0)
                row_pos = lax.broadcasted_iota(jnp.int32, (span, TILE), 1) + (r * TILE) % half
                scores = jnp.where(key_pos <= row_pos + task * half, scores, neg_fill)
            old_max = m_ref[:, cols]
            new_max = jnp.maximum(old_max, jnp.max(scores, axis=0, keepdims=True))
            weights = jnp.exp2(scores - new_max)
            factor = jnp.exp2(old_max - new_max)
            l_ref[:, cols] = l_ref[:, cols] * factor + jnp.sum(weights, axis=0, keepdims=True)
            m_ref[:, cols] = new_max
            acc_ref[:, cols] = acc_ref[:, cols] * factor + jnp.dot(
                values_t, weights.astype(jnp.bfloat16), preferred_element_type=jnp.float32
            )
            if not last:
                s_ref[:, cols] = following

    def one_task(t, _):
        m_ref[...] = jnp.full_like(m_ref, neg_fill)
        l_ref[...] = jnp.zeros_like(l_ref)
        acc_ref[...] = jnp.zeros_like(acc_ref)

        @pl.when((diag[t] > 0) | (lo[t] < hi[t]))
        def _():
            keys = keys_twice(lo[t])
            for cols in tiles:
                s_ref[:, cols] = scores_of(keys, t, cols)

        def body(at_span, _):
            step(t, at_span, False)
            return 0

        lax.fori_loop(lo[t], hi[t], body, 0)

        @pl.when(diag[t] > 0)
        def _():
            step(t, hi[t], True)

        total = l_ref[...]
        some = total > 0.0
        safe = jnp.where(some, total, 1.0)
        lse_ref[t] = jnp.where(some, m_ref[...] + jnp.log2(safe), neg_fill)
        out = acc_ref[...] / safe
        for h in range(2):
            out_ref[t, :, h * HD : (h + 1) * HD] = out[:, h * half : (h + 1) * half].T.astype(
                out_ref.dtype
            )
        return 0

    lax.fori_loop(0, tasks, one_task, 0)


def attend(lo, hi, diag, slots, q, pieces):
    tasks, _, rows = q.shape
    smem = pl.BlockSpec(memory_space=pltpu.SMEM)
    vmem = pl.BlockSpec(memory_space=pltpu.VMEM)
    hbm = pl.BlockSpec(memory_space=pltpu.MemorySpace.HBM)
    return pl.pallas_call(
        attend_kernel,
        out_shape=(
            jax.ShapeDtypeStruct((tasks, rows // 2, PAIR), jnp.bfloat16),
            jax.ShapeDtypeStruct((tasks, 1, rows), jnp.float32),
        ),
        in_specs=[smem] * 4 + [vmem] + [hbm] * len(pieces),
        out_specs=(vmem, vmem),
        scratch_shapes=[
            pltpu.VMEM((16,) + pieces[0].shape, jnp.bfloat16),
            pltpu.VMEM((pieces[0].shape[0] // 2, rows), jnp.float32),
            pltpu.VMEM((1, rows), jnp.float32),
            pltpu.VMEM((1, rows), jnp.float32),
            pltpu.VMEM((HD, rows), jnp.float32),
            pltpu.SemaphoreType.DMA((len(pieces),)),
        ],
        compiler_params=pltpu.CompilerParams(vmem_limit_bytes=48 * 2**20),
        cost_estimate=pl.CostEstimate(
            flops=16384 * 1024 * HD * 4, bytes_accessed=9_000_000, transcendentals=0
        ),
    )(lo, hi, diag, slots, q, *pieces)


def project_kernel(at, low_ref, high_ref, *refs):
    weights, (keep, out_z, out_c, out_cz, acc) = refs[:8], refs[8:]
    acc[...] = jnp.dot(
        jnp.concatenate([low_ref[...], high_ref[...]], axis=1),
        jnp.concatenate([w[...] for w in weights[::2] + weights[1::2]], axis=0),
        preferred_element_type=jnp.float32,
    )
    count = acc.shape[0] // 4
    block = lambda i: acc[pl.ds(pl.multiple_of(at[i] * count, count), count), :]
    keep[...] = block(0)
    out_z[...] = block(1).astype(jnp.bfloat16)
    out_c[...] = block(2).astype(jnp.bfloat16)
    out_cz[...] = block(3).astype(jnp.bfloat16)


def project(at, low, high, *weights):
    rows, width = low.shape[0], weights[0].shape[1]
    tile = 384
    whole = pl.BlockSpec(low.shape, lambda n: (0, 0))
    weight = pl.BlockSpec((PAIR, tile), lambda n: (0, n))
    out = pl.BlockSpec((rows // 4, tile), lambda n: (0, n))
    sent = jax.ShapeDtypeStruct((rows // 4, width), jnp.bfloat16)
    return pl.pallas_call(
        project_kernel,
        grid=(width // tile,),
        out_shape=(jax.ShapeDtypeStruct((rows // 4, width), jnp.float32), sent, sent, sent),
        in_specs=[pl.BlockSpec(memory_space=pltpu.SMEM), whole, whole] + [weight] * 8,
        out_specs=(out,) * 4,
        scratch_shapes=[pltpu.VMEM((rows, tile), jnp.float32)],
        cost_estimate=pl.CostEstimate(
            flops=rows * 2048 * width * 2, bytes_accessed=12_000_000, transcendentals=0
        ),
    )(at, low, high, *weights)


def packed_queries(q):
    tokens = q.shape[0]
    scaled = q.astype(jnp.float32) * query_scale
    scaled = scaled.reshape(tokens, 2, HD).transpose(2, 1, 0).reshape(HD, 2 * tokens)
    high = lax.reduce_precision(scaled, 8, 7)
    low = scaled - high
    return jnp.concatenate([high, low], axis=0).astype(jnp.bfloat16)


def values_in_blocks(v):
    tokens = v.shape[0]
    return v.reshape(tokens // HD, HD, HD).transpose(0, 2, 1).reshape(tokens, HD)


def layer(queries, key_rows, values, out_weight):
    core = lax.axis_index("c")
    x = lax.axis_index("x")
    zl = lax.axis_index("zl")
    spans_y, spans_z = lax.axis_size("y"), lax.axis_size("zh")
    spans = spans_y * spans_z
    span = lax.axis_index("y") * spans_z + lax.axis_index("zh")
    rows = queries.shape[0]
    width = out_weight.shape[1]
    half_width = width // 2

    mine = jnp.concatenate(
        [
            lax.dynamic_slice_in_dim(queries, core * PAIR, PAIR, 1),
            lax.dynamic_slice_in_dim(key_rows, core * HD, HD, 1),
            lax.dynamic_slice_in_dim(values, core * HD, HD, 1),
        ],
        axis=1,
    )
    theirs = jnp.concatenate(
        [
            lax.dynamic_slice_in_dim(queries, (1 - core) * PAIR, PAIR, 1),
            lax.dynamic_slice_in_dim(key_rows, (1 - core) * HD, HD, 1),
            lax.dynamic_slice_in_dim(values, (1 - core) * HD, HD, 1),
        ],
        axis=1,
    )
    got = moved(theirs, "c", lambda at: (1 - at[0],))
    first = jnp.where(core == 0, mine, got)
    second = jnp.where(core == 0, got, mine)

    kv_own = jnp.concatenate(
        [
            first[:, PAIR : PAIR + HD],
            second[:, PAIR : PAIR + HD],
            values_in_blocks(first[:, PAIR + HD :]),
            values_in_blocks(second[:, PAIR + HD :]),
        ],
        axis=0,
    )
    y_up = lambda a: moved(a, "y", lambda at: (at[0] + 1,))
    y_down = lambda a: moved(a, "y", lambda at: (at[0] - 1,))
    z_up = lambda a: moved(a, "zh", lambda at: (at[0] + 1,))
    z_down = lambda a: moved(a, "zh", lambda at: (at[0] - 1,))
    own_kv, out_weight = lax.optimization_barrier((kv_own, out_weight))
    size = own_kv.shape[0] // 2
    z1, z3 = z_up(own_kv), z_down(own_kv)
    y1, y3 = y_up(own_kv), y_down(own_kv)
    x_up = lambda a: moved(a, "x", lambda at: (at[0] + 1,))
    x_down = lambda a: moved(a, "x", lambda at: (at[0] - 1,))
    own_w = lax.dynamic_slice_in_dim(out_weight, core * half_width, half_width, 1)
    w0 = (own_w[:PAIR], own_w[PAIR:])
    w1_top, w3_low = x_up(w0[0]), x_down(w0[1])
    w1_low, w3_top = x_up(w0[1]), x_down(w0[0])

    y2 = [y_up(y1[:size]), y_down(y3[size:])]
    y2 = jnp.concatenate(y2, axis=0)
    z1, z3, y1, y3, y2, lending = lax.optimization_barrier(
        (z1, z3, y1, y3, y2, second[:, :PAIR])
    )
    z1_up, z1_down = y_up(z1), y_down(z1)
    z3_up, z3_down = y_up(z3), y_down(z3)
    z2 = [z_up(z1[:size]), z_down(z3[size:])]
    z2 = jnp.concatenate(z2, axis=0)
    mirror = lambda at: (spans_y - 1 - at[0], spans_z - 1 - at[1])
    lent = moved(lending, ("y", "zh"), mirror)
    z2, y2 = lax.optimization_barrier((z2, y2))
    z2_up, z2_down = y_up(z2), y_down(z2)
    z1_far, z3_far = z_up(y2), z_down(y2)
    pieces = [own_kv, y1, y3, y2]
    pieces += [z1, z1_up, z1_down, z1_far]
    pieces += [z3, z3_up, z3_down, z3_far]
    pieces += [z2, z2_up, z2_down, y_up(z2_up[:size]), y_down(z2_down[size:])]
    w1_top, w3_low, *_ = lax.optimization_barrier(
        (w1_top, w3_low, z1_up, z1_down, z3_up, z3_down)
    )
    w2_top = x_up(w1_top)
    w2_low = x_down(w3_low)

    lent_len = jnp.maximum(2 * span - (spans - 1), 0)
    taken_len = jnp.maximum(spans - 1 - 2 * span, 0)
    ints = lambda *v: jnp.stack([jnp.asarray(e, jnp.int32) for e in v])
    order = jnp.arange(spans, dtype=jnp.int32)
    slots = (lax.axis_index("y") - order // spans_z) % spans_y * 4
    slots = (slots + (lax.axis_index("zh") - order % spans_z) % spans_z).astype(jnp.int32)
    q_all = jnp.stack([packed_queries(a) for a in (first[:, :PAIR], second[:, :PAIR], lent)])
    out, lse = attend(
        ints(0, lent_len, 0), ints(span, span, taken_len), ints(1, 1, 0), slots, q_all, pieces
    )
    back_out = moved(out[2], ("y", "zh"), mirror)
    back_lse = moved(lse[2], ("y", "zh"), mirror)
    back_lse = jnp.where(lent_len > 0, back_lse[0], neg_fill)
    joint = jnp.maximum(lse[1, 0], back_lse)
    own_part = jnp.exp2(lse[1, 0] - joint)
    back_part = jnp.exp2(back_lse - joint)
    total = own_part + back_part

    def by_row(a):
        return jnp.repeat(a.reshape(2, rows).T, HD, axis=1)

    merged = out[1].astype(jnp.float32) * by_row(own_part / total) + back_out.astype(
        jnp.float32
    ) * by_row(back_part / total)
    attended = jnp.stack([out[0], merged.astype(jnp.bfloat16)])

    groups = lax.axis_size("x")
    piece = rows // groups
    by_x = attended.reshape(2, groups, piece, PAIR).transpose(1, 0, 2, 3)
    by_x = by_x.reshape(groups, 2 * piece, PAIR)

    def towards(k):
        block = lax.dynamic_index_in_dim(by_x, (x + k) % groups, 0, keepdims=False)
        return block if k == 0 else moved(block, "x", lambda at: (at[0] + k,))

    heads_mine = jnp.concatenate([towards(k) for k in range(groups)], axis=1)
    heads_other = moved(heads_mine, "c", lambda at: (1 - at[0],))
    low = jnp.where(core == 0, heads_mine, heads_other)
    high = jnp.where(core == 0, heads_other, heads_mine)
    blocks = ints(core * 2 + zl, core * 2 + 1 - zl, 2 - core * 2 + zl, 2 - core * 2 + 1 - zl)
    keep, send_z, send_c, send_cz = project(
        blocks, low, high, *w0, w1_top, w1_low, w2_top, w2_low, w3_top, w3_low
    )
    got_z = moved(send_z, "zl", lambda at: (1 - at[0],))
    got_cz = moved(send_cz, ("c", "zl"), lambda at: (1 - at[0], 1 - at[1]))
    got_c = moved(send_c, "c", lambda at: (1 - at[0],))
    mine_cols = (keep + got_z.astype(jnp.float32)).astype(jnp.bfloat16)
    other_cols = (got_c.astype(jnp.float32) + got_cz.astype(jnp.float32)).astype(jnp.bfloat16)
    return jnp.where(
        core == 0,
        jnp.concatenate([mine_cols, other_cols], axis=1),
        jnp.concatenate([other_cols, mine_cols], axis=1),
    )


def solution(mesh):
    names = ("y", "zh", "c", "x", "zl")
    torus = Mesh(mesh.devices.reshape(4, 4, 2, 4, 2), names)
    seq, head = ("y", "zh", "c"), ("x", "zl")
    in_specs = (P(seq, head), P(seq, head), P(seq, head), P(head, None))
    out_specs = P(seq + head, None)
    return jax.shard_map(layer, mesh=torus, in_specs=in_specs, out_specs=out_specs, check_vma=False)
```

```python
import functools

import jax
import jax.numpy as jnp
from jax import lax
from jax.experimental import pallas as pl
from jax.experimental.pallas import tpu as pltpu
from jax.sharding import Mesh
from jax.sharding import PartitionSpec as P

HD = 128
PAIR = 2 * HD
LOG2E = 1.4426950408889634
query_scale = 168.0 ** (-0.5) * LOG2E
neg_fill = -1e30
TILE = 256
PLACES = (
    [(4 * dy, 0) for dy in (0, 1, 3, 2)]
    + [(4 * dy + dz, 0) for dz in (1, 3) for dy in (0, 1, 3, 2)]
    + [(4 * dy + 2, 0) for dy in (0, 1, 3)]
    + [(10, 0), (10, 1)]
)


def moved(value, axes, mapping):
    names = axes if isinstance(axes, tuple) else (axes,)
    sizes = [lax.axis_size(name) for name in names]
    pairs = []
    total = 1
    for size in sizes:
        total *= size
    for source in range(total):
        coords, rest = [], source
        for size in reversed(sizes):
            coords.append(rest % size)
            rest //= size
        target = 0
        for size, at in zip(sizes, mapping(tuple(reversed(coords)))):
            target = target * size + at % size
        pairs.append((source, target))
    return lax.ppermute(value, axes, pairs)


def attend_kernel(lo, hi, slots, q_ref, *refs, masked):
    pieces, (out_ref, lse_ref, kv_ref, qt_ref, s_ref, m_ref, l_ref, acc_ref, sems) = refs[:-9], refs[-9:]
    tasks, half, _ = q_ref.shape
    rows = 2 * half
    span = kv_ref.shape[1] // 2

    copies = [
        pltpu.make_async_copy(
            piece, kv_ref.at[slot, pl.ds(part * span, piece.shape[0]), :], sems.at[i]
        )
        for i, (piece, (slot, part)) in enumerate(zip(pieces, PLACES))
    ]
    for copy in copies:
        copy.start()

    def pack(t, _):
        for h in range(2):
            cols = pl.ds(h * half, half)
            scaled = q_ref[t, :, h * HD : (h + 1) * HD].astype(jnp.float32) * query_scale
            scaled = scaled.T
            high = scaled.astype(jnp.bfloat16)
            qt_ref[t, :HD, cols] = high
            qt_ref[t, HD:, cols] = (scaled - high.astype(jnp.float32)).astype(jnp.bfloat16)
        return 0

    lax.fori_loop(0, tasks, pack, 0)
    for copy in copies:
        copy.wait()

    tiles = [pl.ds(r * TILE, TILE) for r in range(rows // TILE)]

    def keys_twice(at_span):
        keys = kv_ref[slots[at_span], pl.ds(0, span), :]
        return jnp.concatenate([keys, keys], axis=1)

    def scores_of(keys, task, cols):
        return jnp.dot(keys, qt_ref[task, :, cols], preferred_element_type=jnp.float32)

    def step(task, at_span, last):
        slot = slots[at_span]
        values_t = jnp.concatenate(
            [kv_ref[slot, pl.ds(span + i * HD, HD), :] for i in range(span // HD)], axis=1
        )

        def absorb(scores, cols):
            old_max = m_ref[:, cols]
            new_max = jnp.maximum(old_max, jnp.max(scores, axis=0, keepdims=True))
            weights = jnp.exp2(scores - new_max)
            factor = jnp.exp2(old_max - new_max)
            l_ref[:, cols] = l_ref[:, cols] * factor + jnp.sum(weights, axis=0, keepdims=True)
            m_ref[:, cols] = new_max
            acc_ref[:, cols] = acc_ref[:, cols] * factor + jnp.dot(
                values_t, weights.astype(jnp.bfloat16), preferred_element_type=jnp.float32
            )

        if last:
            key_pos = lax.broadcasted_iota(jnp.int32, (span, half), 0)
            row_pos = lax.broadcasted_iota(jnp.int32, (span, half), 1) + task * half

            def head(h, _):
                cols = pl.ds(pl.multiple_of(h * half, half), half)
                absorb(jnp.where(key_pos <= row_pos, s_ref[:, cols], neg_fill), cols)
                return 0

            lax.fori_loop(0, 2, head, 0)
        else:
            keys = keys_twice(at_span + 1)
            for cols in tiles:
                scores = s_ref[:, cols]
                following = scores_of(keys, task, cols)
                absorb(scores, cols)
                s_ref[:, cols] = following

    def one_task(t, _):
        m_ref[...] = jnp.full_like(m_ref, neg_fill)
        l_ref[...] = jnp.zeros_like(l_ref)
        acc_ref[...] = jnp.zeros_like(acc_ref)

        @pl.when(masked | (lo[t] < hi[t]))
        def _():
            keys = keys_twice(lo[t])

            def fill(r, _):
                cols = pl.ds(pl.multiple_of(r * TILE, TILE), TILE)
                s_ref[:, cols] = scores_of(keys, t, cols)
                return 0

            lax.fori_loop(0, rows // TILE, fill, 0)

        def body(at_span, _):
            step(t, at_span, False)
            return 0

        lax.fori_loop(lo[t], hi[t], body, 0)

        if masked:
            step(t, hi[t], True)

        total = l_ref[...]
        some = total > 0.0
        safe = jnp.where(some, total, 1.0)
        lse_ref[t] = jnp.where(some, m_ref[...] + jnp.log2(safe), neg_fill)
        out = acc_ref[...] / safe
        for h in range(2):
            out_ref[t, :, h * HD : (h + 1) * HD] = out[:, h * half : (h + 1) * half].T.astype(
                out_ref.dtype
            )
        return 0

    lax.fori_loop(0, tasks, one_task, 0)


def attend(lo, hi, slots, q, pieces, masked):
    tasks, rows = q.shape[0], 2 * q.shape[1]
    smem = pl.BlockSpec(memory_space=pltpu.SMEM)
    vmem = pl.BlockSpec(memory_space=pltpu.VMEM)
    hbm = pl.BlockSpec(memory_space=pltpu.MemorySpace.HBM)
    return pl.pallas_call(
        functools.partial(attend_kernel, masked=masked),
        out_shape=(
            jax.ShapeDtypeStruct((tasks, rows // 2, PAIR), jnp.bfloat16),
            jax.ShapeDtypeStruct((tasks, 1, rows), jnp.float32),
        ),
        in_specs=[smem] * 3 + [vmem] + [hbm] * len(pieces),
        out_specs=(vmem, vmem),
        scratch_shapes=[
            pltpu.VMEM((16,) + pieces[0].shape, jnp.bfloat16),
            pltpu.VMEM((tasks, PAIR, rows), jnp.bfloat16),
            pltpu.VMEM((pieces[0].shape[0] // 2, rows), jnp.float32),
            pltpu.VMEM((1, rows), jnp.float32),
            pltpu.VMEM((1, rows), jnp.float32),
            pltpu.VMEM((HD, rows), jnp.float32),
            pltpu.SemaphoreType.DMA((len(pieces),)),
        ],
        compiler_params=pltpu.CompilerParams(vmem_limit_bytes=48 * 2**20),
        cost_estimate=pl.CostEstimate(
            flops=8192 * 1024 * HD * 4, bytes_accessed=9_000_000, transcendentals=0
        ),
    )(lo, hi, slots, q, *pieces)


def project_kernel(at, low_ref, high_ref, *refs):
    weights, (keep, out_z, out_c, out_cz, acc) = refs[:8], refs[8:]
    acc[...] = jnp.dot(
        jnp.concatenate([low_ref[...], high_ref[...]], axis=1),
        jnp.concatenate([w[...] for w in weights[::2] + weights[1::2]], axis=0),
        preferred_element_type=jnp.float32,
    )
    count = acc.shape[0] // 4
    block = lambda i: acc[pl.ds(pl.multiple_of(at[i] * count, count), count), :]
    keep[...] = block(0)
    out_z[...] = block(1).astype(jnp.bfloat16)
    out_c[...] = block(2).astype(jnp.bfloat16)
    out_cz[...] = block(3).astype(jnp.bfloat16)


def project(at, low, high, *weights):
    rows, width = low.shape[0], weights[0].shape[1]
    tile = width // 3
    whole = pl.BlockSpec(low.shape, lambda n: (0, 0))
    weight = pl.BlockSpec((PAIR, tile), lambda n: (0, n))
    out = pl.BlockSpec((rows // 4, tile), lambda n: (0, n))
    sent = jax.ShapeDtypeStruct((rows // 4, width), jnp.bfloat16)
    return pl.pallas_call(
        project_kernel,
        grid=(width // tile,),
        out_shape=(jax.ShapeDtypeStruct((rows // 4, width), jnp.float32), sent, sent, sent),
        in_specs=[pl.BlockSpec(memory_space=pltpu.SMEM), whole, whole] + [weight] * 8,
        out_specs=(out,) * 4,
        scratch_shapes=[pltpu.VMEM((rows, tile), jnp.float32)],
        cost_estimate=pl.CostEstimate(
            flops=rows * 2048 * width * 2, bytes_accessed=12_000_000, transcendentals=0
        ),
    )(at, low, high, *weights)


def values_in_blocks(v):
    tokens = v.shape[0]
    return v.reshape(tokens // HD, HD, HD).transpose(0, 2, 1).reshape(tokens, HD)


def layer(queries, key_rows, values, out_weight):
    core = lax.axis_index("c")
    x = lax.axis_index("x")
    zl = lax.axis_index("zl")
    spans_y, spans_z = lax.axis_size("y"), lax.axis_size("zh")
    spans = spans_y * spans_z
    span = lax.axis_index("y") * spans_z + lax.axis_index("zh")
    rows = queries.shape[0]
    width = out_weight.shape[1]
    half_width = width // 2

    mine = jnp.concatenate(
        [
            lax.dynamic_slice_in_dim(queries, core * PAIR, PAIR, 1),
            lax.dynamic_slice_in_dim(key_rows, core * HD, HD, 1),
            lax.dynamic_slice_in_dim(values, core * HD, HD, 1),
        ],
        axis=1,
    )
    theirs = jnp.concatenate(
        [
            lax.dynamic_slice_in_dim(queries, (1 - core) * PAIR, PAIR, 1),
            lax.dynamic_slice_in_dim(key_rows, (1 - core) * HD, HD, 1),
            lax.dynamic_slice_in_dim(values, (1 - core) * HD, HD, 1),
        ],
        axis=1,
    )
    got = moved(theirs, "c", lambda at: (1 - at[0],))
    first = jnp.where(core == 0, mine, got)
    second = jnp.where(core == 0, got, mine)

    kv_own = jnp.concatenate(
        [
            first[:, PAIR : PAIR + HD],
            second[:, PAIR : PAIR + HD],
            values_in_blocks(first[:, PAIR + HD :]),
            values_in_blocks(second[:, PAIR + HD :]),
        ],
        axis=0,
    )
    y_up = lambda a: moved(a, "y", lambda at: (at[0] + 1,))
    y_down = lambda a: moved(a, "y", lambda at: (at[0] - 1,))
    z_up = lambda a: moved(a, "zh", lambda at: (at[0] + 1,))
    z_down = lambda a: moved(a, "zh", lambda at: (at[0] - 1,))
    own_kv, out_weight = lax.optimization_barrier((kv_own, out_weight))
    size = own_kv.shape[0] // 2
    z1, z3 = z_up(own_kv), z_down(own_kv)
    y1, y3 = y_up(own_kv), y_down(own_kv)
    x_up = lambda a: moved(a, "x", lambda at: (at[0] + 1,))
    x_down = lambda a: moved(a, "x", lambda at: (at[0] - 1,))
    own_w = lax.dynamic_slice_in_dim(out_weight, core * half_width, half_width, 1)
    w0 = (own_w[:PAIR], own_w[PAIR:])
    w1_top, w3_low = x_up(w0[0]), x_down(w0[1])
    w1_low, w3_top = x_up(w0[1]), x_down(w0[0])

    y2 = [y_up(y1[:size]), y_down(y3[size:])]
    y2 = jnp.concatenate(y2, axis=0)
    z1, z3, y1, y3, y2, lending = lax.optimization_barrier(
        (z1, z3, y1, y3, y2, second[:, :PAIR])
    )
    z1_up, z1_down = y_up(z1), y_down(z1)
    z3_up, z3_down = y_up(z3), y_down(z3)
    z2 = [z_up(z1[:size]), z_down(z3[size:])]
    z2 = jnp.concatenate(z2, axis=0)
    mirror = lambda at: (spans_y - 1 - at[0], spans_z - 1 - at[1])
    lent = moved(lending, ("y", "zh"), mirror)
    z2, y2 = lax.optimization_barrier((z2, y2))
    z2_up, z2_down = y_up(z2), y_down(z2)
    z1_far, z3_far = z_up(y2), z_down(y2)
    pieces = [own_kv, y1, y3, y2]
    pieces += [z1, z1_up, z1_down, z1_far]
    pieces += [z3, z3_up, z3_down, z3_far]
    pieces += [z2, z2_up, z2_down, y_up(z2_up[:size]), y_down(z2_down[size:])]
    w1_top, w3_low, *_ = lax.optimization_barrier(
        (w1_top, w3_low, z1_up, z1_down, z3_up, z3_down)
    )
    w2_top = x_up(w1_top)
    w2_low = x_down(w3_low)

    late = span >= spans // 2
    early_keys = jnp.abs(2 * span - (spans - 1))
    ints = lambda *v: jnp.stack([jnp.asarray(e, jnp.int32) for e in v])
    order = jnp.arange(spans, dtype=jnp.int32)
    slots = (lax.axis_index("y") - order // spans_z) % spans_y * 4
    slots = (slots + (lax.axis_index("zh") - order % spans_z) % spans_z).astype(jnp.int32)
    q_first, q_second = first[:, :PAIR], second[:, :PAIR]
    part_out, part_lse = attend(
        ints(0), ints(early_keys), slots, jnp.where(late, q_first, lent)[None], pieces, False
    )
    back_out = moved(part_out[0], ("y", "zh"), mirror)
    back_lse = moved(part_lse[0], ("y", "zh"), mirror)
    begin = jnp.where(late, early_keys, 0)
    out, lse = attend(
        ints(begin, begin), ints(span, span), slots, jnp.stack([q_first, q_second]), pieces, True
    )
    part_lse = jnp.stack([part_lse[0, 0], back_lse[0]])
    part_lse = jnp.where(late, part_lse, neg_fill)
    lse = lse[:, 0]
    joint = jnp.maximum(lse, part_lse)
    own_share, part_share = jnp.exp2(lse - joint), jnp.exp2(part_lse - joint)
    total = own_share + part_share

    def by_row(a):
        return jnp.repeat(a.reshape(2, 2, rows).transpose(0, 2, 1), HD, axis=2)

    merged = out.astype(jnp.float32) * by_row(own_share / total)
    merged = merged + jnp.stack([part_out[0], back_out]).astype(jnp.float32) * by_row(part_share / total)
    attended = merged.astype(jnp.bfloat16)

    groups = lax.axis_size("x")
    piece = rows // groups
    by_x = attended.reshape(2, groups, piece, PAIR).transpose(1, 0, 2, 3)
    by_x = by_x.reshape(groups, 2 * piece, PAIR)

    def towards(k):
        block = lax.dynamic_index_in_dim(by_x, (x + k) % groups, 0, keepdims=False)
        return block if k == 0 else moved(block, "x", lambda at: (at[0] + k,))

    heads_mine = jnp.concatenate([towards(k) for k in range(groups)], axis=1)
    heads_other = moved(heads_mine, "c", lambda at: (1 - at[0],))
    low = jnp.where(core == 0, heads_mine, heads_other)
    high = jnp.where(core == 0, heads_other, heads_mine)
    blocks = ints(core * 2 + zl, core * 2 + 1 - zl, 2 - core * 2 + zl, 2 - core * 2 + 1 - zl)
    keep, send_z, send_c, send_cz = project(
        blocks, low, high, *w0, w1_top, w1_low, w2_top, w2_low, w3_top, w3_low
    )
    got_z = moved(send_z, "zl", lambda at: (1 - at[0],))
    got_cz = moved(send_cz, ("c", "zl"), lambda at: (1 - at[0], 1 - at[1]))
    got_c = moved(send_c, "c", lambda at: (1 - at[0],))
    mine_cols = (keep + got_z.astype(jnp.float32)).astype(jnp.bfloat16)
    other_cols = (got_c.astype(jnp.float32) + got_cz.astype(jnp.float32)).astype(jnp.bfloat16)
    return jnp.where(
        core == 0,
        jnp.concatenate([mine_cols, other_cols], axis=1),
        jnp.concatenate([other_cols, mine_cols], axis=1),
    )


def solution(mesh):
    names = ("y", "zh", "c", "x", "zl")
    torus = Mesh(mesh.devices.reshape(4, 4, 2, 4, 2), names)
    seq, head = ("y", "zh", "c"), ("x", "zl")
    in_specs = (P(seq, head), P(seq, head), P(seq, head), P(head, None))
    out_specs = P(seq + head, None)
    return jax.shard_map(layer, mesh=torus, in_specs=in_specs, out_specs=out_specs, check_vma=False)
```

```python
import jax
import jax.numpy as jnp
from jax import lax
from jax.experimental import pallas as pl
from jax.experimental.pallas import tpu as pltpu
from jax.sharding import Mesh
from jax.sharding import PartitionSpec as P

HD = 128
PAIR = 2 * HD
LOG2E = 1.4426950408889634
query_scale = 168.0 ** (-0.5) * LOG2E
neg_fill = -1e30
TILE = 256
PLACES = (
    [(4 * dy, 0) for dy in (0, 1, 3, 2)]
    + [(4 * dy + dz, 0) for dz in (1, 3) for dy in (0, 1, 3, 2)]
    + [(4 * dy + 2, 0) for dy in (0, 1, 3)]
    + [(10, 0), (10, 1)]
)


def moved(value, axes, mapping):
    names = axes if isinstance(axes, tuple) else (axes,)
    sizes = [lax.axis_size(name) for name in names]
    pairs = []
    total = 1
    for size in sizes:
        total *= size
    for source in range(total):
        coords, rest = [], source
        for size in reversed(sizes):
            coords.append(rest % size)
            rest //= size
        target = 0
        for size, at in zip(sizes, mapping(tuple(reversed(coords)))):
            target = target * size + at % size
        pairs.append((source, target))
    return lax.ppermute(value, axes, pairs)


def attend_kernel(lo, hi, diag, slots, q_ref, *refs):
    pieces, (out_ref, lse_ref, kv_ref, qt_ref, s_ref, m_ref, l_ref, acc_ref, sems) = refs[:-9], refs[-9:]
    tasks, half, _ = q_ref.shape
    rows = 2 * half
    span = kv_ref.shape[1] // 2

    copies = [
        pltpu.make_async_copy(
            piece, kv_ref.at[slot, pl.ds(part * span, piece.shape[0]), :], sems.at[i]
        )
        for i, (piece, (slot, part)) in enumerate(zip(pieces, PLACES))
    ]
    for copy in copies:
        copy.start()

    def pack(t, _):
        for h in range(2):
            cols = pl.ds(h * half, half)
            scaled = q_ref[t, :, h * HD : (h + 1) * HD].astype(jnp.float32) * query_scale
            scaled = scaled.T
            high = scaled.astype(jnp.bfloat16)
            qt_ref[t, :HD, cols] = high
            qt_ref[t, HD:, cols] = (scaled - high.astype(jnp.float32)).astype(jnp.bfloat16)
        return 0

    lax.fori_loop(0, tasks, pack, 0)
    for copy in copies:
        copy.wait()

    tiles = [pl.ds(r * TILE, TILE) for r in range(rows // TILE)]

    def keys_twice(at_span):
        keys = kv_ref[slots[at_span], pl.ds(0, span), :]
        return jnp.concatenate([keys, keys], axis=1)

    def scores_of(keys, task, cols):
        return jnp.dot(keys, qt_ref[task, :, cols], preferred_element_type=jnp.float32)

    def step(task, at_span, last):
        slot = slots[at_span]
        values_t = jnp.concatenate(
            [kv_ref[slot, pl.ds(span + i * HD, HD), :] for i in range(span // HD)], axis=1
        )
        keys = None if last else keys_twice(at_span + 1)
        for r, cols in enumerate(tiles):
            scores = s_ref[:, cols]
            following = None if last else scores_of(keys, task, cols)
            if last:
                key_pos = lax.broadcasted_iota(jnp.int32, (span, TILE), 0)
                row_pos = lax.broadcasted_iota(jnp.int32, (span, TILE), 1) + (r * TILE) % half
                scores = jnp.where(key_pos <= row_pos + task * half, scores, neg_fill)
            old_max = m_ref[:, cols]
            new_max = jnp.maximum(old_max, jnp.max(scores, axis=0, keepdims=True))
            weights = jnp.exp2(scores - new_max)
            factor = jnp.exp2(old_max - new_max)
            l_ref[:, cols] = l_ref[:, cols] * factor + jnp.sum(weights, axis=0, keepdims=True)
            m_ref[:, cols] = new_max
            acc_ref[:, cols] = acc_ref[:, cols] * factor + jnp.dot(
                values_t, weights.astype(jnp.bfloat16), preferred_element_type=jnp.float32
            )
            if not last:
                s_ref[:, cols] = following

    def one_task(t, _):
        m_ref[...] = jnp.full_like(m_ref, neg_fill)
        l_ref[...] = jnp.zeros_like(l_ref)
        acc_ref[...] = jnp.zeros_like(acc_ref)

        @pl.when((diag[t] > 0) | (lo[t] < hi[t]))
        def _():
            keys = keys_twice(lo[t])
            for cols in tiles:
                s_ref[:, cols] = scores_of(keys, t, cols)

        def body(at_span, _):
            step(t, at_span, False)
            return 0

        lax.fori_loop(lo[t], hi[t], body, 0)

        @pl.when(diag[t] > 0)
        def _():
            step(t, hi[t], True)

        total = l_ref[...]
        some = total > 0.0
        safe = jnp.where(some, total, 1.0)
        lse_ref[t] = jnp.where(some, m_ref[...] + jnp.log2(safe), neg_fill)
        out = acc_ref[...] / safe
        for h in range(2):
            out_ref[t, :, h * HD : (h + 1) * HD] = out[:, h * half : (h + 1) * half].T.astype(
                out_ref.dtype
            )
        return 0

    lax.fori_loop(0, tasks, one_task, 0)


def attend(lo, hi, diag, slots, q, pieces):
    tasks, rows = q.shape[0], 2 * q.shape[1]
    smem = pl.BlockSpec(memory_space=pltpu.SMEM)
    vmem = pl.BlockSpec(memory_space=pltpu.VMEM)
    hbm = pl.BlockSpec(memory_space=pltpu.MemorySpace.HBM)
    return pl.pallas_call(
        attend_kernel,
        out_shape=(
            jax.ShapeDtypeStruct((tasks, rows // 2, PAIR), jnp.bfloat16),
            jax.ShapeDtypeStruct((tasks, 1, rows), jnp.float32),
        ),
        in_specs=[smem] * 4 + [vmem] + [hbm] * len(pieces),
        out_specs=(vmem, vmem),
        scratch_shapes=[
            pltpu.VMEM((16,) + pieces[0].shape, jnp.bfloat16),
            pltpu.VMEM((tasks, PAIR, rows), jnp.bfloat16),
            pltpu.VMEM((pieces[0].shape[0] // 2, rows), jnp.float32),
            pltpu.VMEM((1, rows), jnp.float32),
            pltpu.VMEM((1, rows), jnp.float32),
            pltpu.VMEM((HD, rows), jnp.float32),
            pltpu.SemaphoreType.DMA((len(pieces),)),
        ],
        compiler_params=pltpu.CompilerParams(vmem_limit_bytes=48 * 2**20),
        cost_estimate=pl.CostEstimate(
            flops=16384 * 1024 * HD * 4, bytes_accessed=9_000_000, transcendentals=0
        ),
    )(lo, hi, diag, slots, q, *pieces)


def project_kernel(at, low_ref, high_ref, *refs):
    weights, (keep, out_z, out_c, out_cz, acc) = refs[:8], refs[8:]
    acc[...] = jnp.dot(
        jnp.concatenate([low_ref[...], high_ref[...]], axis=1),
        jnp.concatenate([w[...] for w in weights[::2] + weights[1::2]], axis=0),
        preferred_element_type=jnp.float32,
    )
    count = acc.shape[0] // 4
    block = lambda i: acc[pl.ds(pl.multiple_of(at[i] * count, count), count), :]
    keep[...] = block(0)
    out_z[...] = block(1).astype(jnp.bfloat16)
    out_c[...] = block(2).astype(jnp.bfloat16)
    out_cz[...] = block(3).astype(jnp.bfloat16)


def project(at, low, high, *weights):
    rows, width = low.shape[0], weights[0].shape[1]
    tile = width // 3
    whole = pl.BlockSpec(low.shape, lambda n: (0, 0))
    weight = pl.BlockSpec((PAIR, tile), lambda n: (0, n))
    out = pl.BlockSpec((rows // 4, tile), lambda n: (0, n))
    sent = jax.ShapeDtypeStruct((rows // 4, width), jnp.bfloat16)
    return pl.pallas_call(
        project_kernel,
        grid=(width // tile,),
        out_shape=(jax.ShapeDtypeStruct((rows // 4, width), jnp.float32), sent, sent, sent),
        in_specs=[pl.BlockSpec(memory_space=pltpu.SMEM), whole, whole] + [weight] * 8,
        out_specs=(out,) * 4,
        scratch_shapes=[pltpu.VMEM((rows, tile), jnp.float32)],
        cost_estimate=pl.CostEstimate(
            flops=rows * 2048 * width * 2, bytes_accessed=12_000_000, transcendentals=0
        ),
    )(at, low, high, *weights)


def values_in_blocks(v):
    tokens = v.shape[0]
    return v.reshape(tokens // HD, HD, HD).transpose(0, 2, 1).reshape(tokens, HD)


def layer(queries, key_rows, values, out_weight):
    core = lax.axis_index("c")
    x = lax.axis_index("x")
    zl = lax.axis_index("zl")
    spans_y, spans_z = lax.axis_size("y"), lax.axis_size("zh")
    spans = spans_y * spans_z
    span = lax.axis_index("y") * spans_z + lax.axis_index("zh")
    rows = queries.shape[0]
    width = out_weight.shape[1]
    half_width = width // 2

    mine = jnp.concatenate(
        [
            lax.dynamic_slice_in_dim(queries, core * PAIR, PAIR, 1),
            lax.dynamic_slice_in_dim(key_rows, core * HD, HD, 1),
            lax.dynamic_slice_in_dim(values, core * HD, HD, 1),
        ],
        axis=1,
    )
    theirs = jnp.concatenate(
        [
            lax.dynamic_slice_in_dim(queries, (1 - core) * PAIR, PAIR, 1),
            lax.dynamic_slice_in_dim(key_rows, (1 - core) * HD, HD, 1),
            lax.dynamic_slice_in_dim(values, (1 - core) * HD, HD, 1),
        ],
        axis=1,
    )
    got = moved(theirs, "c", lambda at: (1 - at[0],))
    first = jnp.where(core == 0, mine, got)
    second = jnp.where(core == 0, got, mine)

    kv_own = jnp.concatenate(
        [
            first[:, PAIR : PAIR + HD],
            second[:, PAIR : PAIR + HD],
            values_in_blocks(first[:, PAIR + HD :]),
            values_in_blocks(second[:, PAIR + HD :]),
        ],
        axis=0,
    )
    y_up = lambda a: moved(a, "y", lambda at: (at[0] + 1,))
    y_down = lambda a: moved(a, "y", lambda at: (at[0] - 1,))
    z_up = lambda a: moved(a, "zh", lambda at: (at[0] + 1,))
    z_down = lambda a: moved(a, "zh", lambda at: (at[0] - 1,))
    own_kv, out_weight = lax.optimization_barrier((kv_own, out_weight))
    size = own_kv.shape[0] // 2
    z1, z3 = z_up(own_kv), z_down(own_kv)
    y1, y3 = y_up(own_kv), y_down(own_kv)
    x_up = lambda a: moved(a, "x", lambda at: (at[0] + 1,))
    x_down = lambda a: moved(a, "x", lambda at: (at[0] - 1,))
    own_w = lax.dynamic_slice_in_dim(out_weight, core * half_width, half_width, 1)
    w0 = (own_w[:PAIR], own_w[PAIR:])
    w1_top, w3_low = x_up(w0[0]), x_down(w0[1])
    w1_low, w3_top = x_up(w0[1]), x_down(w0[0])

    y2 = [y_up(y1[:size]), y_down(y3[size:])]
    y2 = jnp.concatenate(y2, axis=0)
    z1, z3, y1, y3, y2, lending = lax.optimization_barrier(
        (z1, z3, y1, y3, y2, second[:, :PAIR])
    )
    z1_up, z1_down = y_up(z1), y_down(z1)
    z3_up, z3_down = y_up(z3), y_down(z3)
    z2 = [z_up(z1[:size]), z_down(z3[size:])]
    z2 = jnp.concatenate(z2, axis=0)
    mirror = lambda at: (spans_y - 1 - at[0], spans_z - 1 - at[1])
    lent = moved(lending, ("y", "zh"), mirror)
    z2_up, z2_down = y_up(z2), y_down(z2)
    z1_far, z3_far = z_up(y2), z_down(y2)
    pieces = [own_kv, y1, y3, y2]
    pieces += [z1, z1_up, z1_down, z1_far]
    pieces += [z3, z3_up, z3_down, z3_far]
    pieces += [z2, z2_up, z2_down, y_up(z2_up[:size]), y_down(z2_down[size:])]
    w1_top, w3_low, *_ = lax.optimization_barrier(
        (w1_top, w3_low, z1_up, z1_down, z3_up, z3_down)
    )
    w2_top = x_up(w1_top)
    w2_low = x_down(w3_low)

    lent_len = jnp.maximum(2 * span - (spans - 1), 0)
    taken_len = jnp.maximum(spans - 1 - 2 * span, 0)
    ints = lambda *v: jnp.stack([jnp.asarray(e, jnp.int32) for e in v])
    order = jnp.arange(spans, dtype=jnp.int32)
    slots = (lax.axis_index("y") - order // spans_z) % spans_y * 4
    slots = (slots + (lax.axis_index("zh") - order % spans_z) % spans_z).astype(jnp.int32)
    q_all = jnp.stack([first[:, :PAIR], second[:, :PAIR], lent])
    out, lse = attend(
        ints(0, lent_len, 0), ints(span, span, taken_len), ints(1, 1, 0), slots, q_all, pieces
    )
    back_out = moved(out[2], ("y", "zh"), mirror)
    back_lse = moved(lse[2], ("y", "zh"), mirror)
    back_lse = jnp.where(lent_len > 0, back_lse[0], neg_fill)
    joint = jnp.maximum(lse[1, 0], back_lse)
    own_part = jnp.exp2(lse[1, 0] - joint)
    back_part = jnp.exp2(back_lse - joint)
    total = own_part + back_part

    def by_row(a):
        return jnp.repeat(a.reshape(2, rows).T, HD, axis=1)

    merged = out[1].astype(jnp.float32) * by_row(own_part / total) + back_out.astype(
        jnp.float32
    ) * by_row(back_part / total)
    attended = jnp.stack([out[0], merged.astype(jnp.bfloat16)])

    groups = lax.axis_size("x")
    piece = rows // groups
    by_x = attended.reshape(2, groups, piece, PAIR).transpose(1, 0, 2, 3)
    by_x = by_x.reshape(groups, 2 * piece, PAIR)

    def towards(k):
        block = lax.dynamic_index_in_dim(by_x, (x + k) % groups, 0, keepdims=False)
        return block if k == 0 else moved(block, "x", lambda at: (at[0] + k,))

    heads_mine = jnp.concatenate([towards(k) for k in range(groups)], axis=1)
    heads_other = moved(heads_mine, "c", lambda at: (1 - at[0],))
    low = jnp.where(core == 0, heads_mine, heads_other)
    high = jnp.where(core == 0, heads_other, heads_mine)
    blocks = ints(core * 2 + zl, core * 2 + 1 - zl, 2 - core * 2 + zl, 2 - core * 2 + 1 - zl)
    keep, send_z, send_c, send_cz = project(
        blocks, low, high, *w0, w1_top, w1_low, w2_top, w2_low, w3_top, w3_low
    )
    got_z = moved(send_z, "zl", lambda at: (1 - at[0],))
    got_cz = moved(send_cz, ("c", "zl"), lambda at: (1 - at[0], 1 - at[1]))
    got_c = moved(send_c, "c", lambda at: (1 - at[0],))
    mine_cols = (keep + got_z.astype(jnp.float32)).astype(jnp.bfloat16)
    other_cols = (got_c.astype(jnp.float32) + got_cz.astype(jnp.float32)).astype(jnp.bfloat16)
    return jnp.where(
        core == 0,
        jnp.concatenate([mine_cols, other_cols], axis=1),
        jnp.concatenate([other_cols, mine_cols], axis=1),
    )


def solution(mesh):
    names = ("y", "zh", "c", "x", "zl")
    torus = Mesh(mesh.devices.reshape(4, 4, 2, 4, 2), names)
    seq, head = ("y", "zh", "c"), ("x", "zl")
    in_specs = (P(seq, head), P(seq, head), P(seq, head), P(head, None))
    out_specs = P(seq + head, None)
    return jax.shard_map(layer, mesh=torus, in_specs=in_specs, out_specs=out_specs, check_vma=False)
```
